32 devices in a mesh: groups: 2 (over y), seq: 4 (over x, core), qset: 4 (over z).
Axes of the slice: x: 2, y: 2, z: 4, core: 2. Of those that a mesh axis runs over, the one named last changes fastest.
Arguments:
- states: bfloat16 [8, 4, 128, 4096], P(('groups', 'qset'), 'seq'), parts along dimension 0, may hold values from -7 to 7
- enc_gain: bfloat16 [4096], replicated, may hold values from 0.25 to 1.75
- dec_states: bfloat16 [16, 64, 4096], P(('groups', 'qset')), parts along dimension 0, may hold values from -7 to 7
- dec_gain: bfloat16 [4096], replicated, may hold values from 0.25 to 1.75
- query_weight: bfloat16 [4096, 4096], P(None, 'seq'), may hold values from -0.375 to 0.375
- key_value_weight: bfloat16 [4096, 2, 4096], P(None, None, 'seq'), may hold values from -0.0625 to 0.0625
- out_weight: bfloat16 [4096, 4096], P('seq'), may hold values from -0.75 to 0.75
- question_of: int32 [8, 4, 1], P('groups'), parts along dimension 0, may hold values from 0 to 7; in each aligned block of 4 rows (0 to 3, 4 to 7, ..., all dimensions but the last counted through in order) at most 2 rows name the same one
Outputs:
- mixed: bfloat16 [16, 64, 4096], P(('groups', 'qset'), None, 'seq'), parts along dimension 0
The draws below stay inside these ranges and needn't reach their ends.
There are 2 independent parts, one for each index of `groups`. The reference program is written for one: setup_inputs(seed, part) draws one part's arguments, and reference() takes and returns one part's arrays. A program takes and returns all parts, laid end to end along the dimension named above; an argument that names none is the same for every part. Nothing has to cross between parts.
Inputs may be any that keep to these rules, and one draw needn't show every extreme that they name: `question_of`: within each index of the first dimension (one source group of 4 passages) at most 2 passages name the same question, and exactly 2 do for some question in some groups; every question is named by at least one passage.
All inputs are finite; a program needn't handle non-finite values.
Results may differ from the reference program's by a relative error of at most 0.014.
The reference program's roundings to bfloat16 on the way count: a program that leaves them out, or rounds other values in their place, can miss the bound.
Values may be sent and summed in bfloat16 or wider, within the bound.
A program may use at most 128 MiB of HBM per device.

```python
import math
import jax
import jax.numpy as jnp
import numpy as np
from jax import lax

D = 4096
HEADS = 64
HD = 64
PLEN = 128
CAP = 2
DTOK = 64
QUESTIONS = 8
N_SEQ = 4
N_QSET = 4


def drawn_rows(salt_key, lead_shape):
    values = jax.random.normal(jax.random.fold_in(salt_key, 105), lead_shape + (D,), jnp.float32)
    return jnp.clip(values, -6.0, 6.0)


def draw_states(key, part):
    salt_key = jax.random.fold_in(key, 11)
    lead_shape = (N_QSET, N_SEQ, PLEN)
    result = drawn_rows(salt_key, lead_shape)
    return result.astype(jnp.bfloat16)


def draw_dec_states(key, part):
    salt_key = jax.random.fold_in(key, 12)
    lead_shape = (QUESTIONS, DTOK)
    result = drawn_rows(salt_key, lead_shape)
    return result.astype(jnp.bfloat16)


def weight_tables(key):
    key_part = jax.random.normal(jax.random.fold_in(key, 201), (D, 2, HEADS * HD), jnp.float32)
    key_part = jnp.clip(key_part, -4.0, 4.0) * D ** (-0.5)
    query_part = jax.random.normal(jax.random.fold_in(key, 202), (D, HEADS * HD), jnp.float32)
    query_part = jnp.clip(query_part, -4.0, 4.0) * (D * HD) ** (-0.5)
    return (key_part, query_part)


def draw_key_value_weight(key, part):
    key_part, query_part = weight_tables(key)
    return key_part.astype(jnp.bfloat16)


def draw_query_weight(key, part):
    key_part, query_part = weight_tables(key)
    result = query_part
    return result.astype(jnp.bfloat16)


def steps_of(own_key, dims, split, low, largest):
    def one(dim, blocks):
        draws = jax.random.uniform(jax.random.fold_in(jax.random.fold_in(own_key, 6), dim), (blocks,), jnp.float32, low / len(split), largest / len(split))
        return jnp.repeat(jnp.exp(draws), dims[dim] // blocks).reshape((-1,) + (1,) * (len(dims) - dim - 1))

    loudness = one(*split[0])
    for cut in split[1:]:
        loudness = loudness * one(*cut)
    return loudness


def shared_out(rng, own, number, rows, amount, top, bound, slope):
    order = jax.random.permutation(rng, amount)
    heavy_load, ordinary = load_shares(amount, rows * top, bound, slope, True), load_shares(amount, rows * top, bound, slope, False)
    places = jnp.arange(amount)

    def named(tallies, offset_by):
        used = int((tallies > 0).sum())
        fixed = max(1, used // 4)
        shifted = fixed + (places - fixed + offset_by * (used - fixed)) % max(1, amount - fixed)
        return jnp.zeros((amount,), jnp.int32).at[order[jnp.where(places < fixed, places, shifted)]].set(jnp.asarray(tallies, jnp.int32))

    tallies = jnp.where(number % 4 == 0, named(heavy_load, number // 4), named(ordinary, number - number // 4 - 1))
    mixed = jax.random.permutation(jax.random.fold_in(own, 3), amount)
    giver, sink = mixed[0:amount // 2 * 2:2], mixed[1:amount // 2 * 2:2]
    room = jnp.minimum(tallies[giver] - 1, bound - tallies[sink]) // 2
    room = jnp.where((giver == order[0]) | (sink == order[0]) | (tallies[sink] == 0), 0, jnp.maximum(room, 0))
    shifted = jax.random.randint(jax.random.fold_in(own, 4), (amount // 2,), 0, 1 << 20) % (room + 1)
    tallies = tallies.at[giver].add(-shifted).at[sink].add(shifted)
    items = jnp.searchsorted(jnp.cumsum(tallies), jnp.arange(rows * top), side="right").astype(jnp.int32)
    table = items.reshape(top, rows).T
    table = table[jax.random.permutation(jax.random.fold_in(own, 1), rows)]
    offset_by = jax.random.randint(jax.random.fold_in(own, 2), (rows, 1), 0, top)
    return jnp.take_along_axis(table, (jnp.arange(top)[None, :] + offset_by) % top, axis=1)


def load_shares(amount, total, reach, skew, full):
    portions = [(1 << 20) // math.isqrt(rank ** skew) + 1 for rank in range(1, amount + 1)]
    largest = reach if full else min(reach, max(-(-total // amount), total * portions[0] // sum(portions)))
    least = 1 if total - largest >= amount - 1 else 0
    given, surplus = [largest] + [least] * (amount - 1), total - largest - least * (amount - 1)
    while surplus > 0:
        movable = [i for i in range(1, amount) if given[i] < largest] or [i for i in range(1, amount) if given[i] < reach]
        whole, budget = sum([portions[i] for i in movable]), surplus
        for i in movable:
            more = min(reach - given[i], max(1, budget * portions[i] // whole), surplus)
            given[i] = given[i] + more
            surplus = surplus - more
    return np.array(given)


def normal_values(rng, shape, width, limit, split=(), held_as=jnp.bfloat16):
    array = jax.random.normal(rng, shape, jnp.float32) * width
    if len(split) > 0:
        array = steps_of(rng, shape, split, -0.22, 0.18) * array
    return jnp.clip(array, min=-limit, max=limit).astype(held_as)


def setup_inputs(seed: int = 0, part: int = 0) -> dict:
    arg_keys = jax.random.split(jax.random.key(seed), 9)
    part_keys = jax.random.split(jax.random.fold_in(arg_keys[8], part), 9)
    states = draw_states(jax.random.fold_in(jax.random.fold_in(arg_keys[8], part), 71), part)
    enc_gain = jnp.clip(1.0 + 0.15 * jax.random.normal(arg_keys[1], (D,), jnp.float32), 0.25, 1.75).astype(jnp.bfloat16)
    dec_states = draw_dec_states(jax.random.fold_in(jax.random.fold_in(arg_keys[8], part), 71), part)
    dec_gain = jnp.clip(1.0 + 0.15 * jax.random.normal(arg_keys[3], (D,), jnp.float32), 0.25, 1.75).astype(jnp.bfloat16)
    query_weight = draw_query_weight(jax.random.fold_in(arg_keys[8], 71), part)
    key_value_weight = draw_key_value_weight(jax.random.fold_in(arg_keys[8], 71), part)
    out_weight = normal_values(arg_keys[6], (HEADS * HD, D), HD ** -0.5, 0.75, ((0, 4),))
    question_of_keys = jax.random.split(jax.random.fold_in(part_keys[7], 1), N_QSET * N_SEQ // N_SEQ)
    question_of_turns = jax.random.permutation(jax.random.fold_in(part_keys[7], 3), N_QSET * N_SEQ // N_SEQ)
    question_of = jax.vmap(lambda own, number: shared_out(jax.random.fold_in(part_keys[7], 2), own, number, N_SEQ, QUESTIONS, 1, CAP, 2))(question_of_keys, question_of_turns).reshape((N_QSET, N_SEQ, 1))
    return {"states": states, "enc_gain": enc_gain, "dec_states": dec_states, "dec_gain": dec_gain, "query_weight": query_weight, "key_value_weight": key_value_weight, "out_weight": out_weight, "question_of": question_of}


EPSILON = 1e-06
MASKED_SCORE = -1e+30

def scaled_norm(rows_in, gain_vec):
    rows_f32 = rows_in.astype(jnp.float32)
    mean_square = lax.optimization_barrier(jnp.mean(rows_f32 * rows_f32, axis=-1, keepdims=True))
    return rows_f32 * lax.rsqrt(mean_square + EPSILON) * gain_vec.astype(jnp.float32)

def rounded(values_in):
    return lax.optimization_barrier(values_in.astype(jnp.bfloat16)).astype(jnp.float32)

def reference(states, enc_gain, dec_states, dec_gain, query_weight, key_value_weight, out_weight, question_of):
    enc_rows = scaled_norm(states, enc_gain).astype(jnp.bfloat16).reshape(-1, D)
    passage_question = question_of.reshape(-1).astype(jnp.int32)
    row_question = jnp.repeat(passage_question, PLEN)
    question_count = dec_states.shape[0]
    live_mask = row_question[None, :] == jnp.arange(question_count, dtype=jnp.int32)[:, None]
    dec_rows = scaled_norm(dec_states, dec_gain).astype(jnp.bfloat16).reshape(-1, D)
    query_heads = jnp.transpose(query_weight.reshape(D, HEADS, HD), (1, 0, 2))
    key_heads = jnp.transpose(key_value_weight[:, 0, :].reshape(D, HEADS, HD), (1, 0, 2))
    value_heads = jnp.transpose(key_value_weight[:, 1, :].reshape(D, HEADS, HD), (1, 0, 2))
    out_heads = out_weight.reshape(HEADS, HD, D)

    def one_head(carry, weights_in):
        w_query, w_key, w_value, w_out = weights_in
        queries = jnp.dot(dec_rows, w_query, preferred_element_type=jnp.float32).astype(jnp.bfloat16)
        key_rows = jnp.dot(enc_rows, w_key, preferred_element_type=jnp.float32).astype(jnp.bfloat16)
        value_rows = jnp.dot(enc_rows, w_value, preferred_element_type=jnp.float32).astype(jnp.bfloat16)
        query_blocks = rounded(queries).reshape(question_count, -1, HD)
        scores = jnp.einsum('qtd,rd->qtr', query_blocks, key_rows.astype(jnp.float32))
        scores = jnp.where(live_mask[:, None, :], scores, MASKED_SCORE)
        row_peak = lax.optimization_barrier(jnp.max(scores, axis=-1, keepdims=True))
        weights = jnp.where(live_mask[:, None, :], jnp.exp(scores - row_peak), 0.0)
        row_total = lax.optimization_barrier(jnp.sum(weights, axis=-1, keepdims=True))
        summed = jnp.einsum('qtr,rd->qtd', rounded(weights), value_rows.astype(jnp.float32))
        attended = (summed / row_total).astype(jnp.bfloat16).reshape(-1, HD)
        return (carry + jnp.dot(attended, w_out, preferred_element_type=jnp.float32), None)
    start_sum = jnp.zeros((dec_rows.shape[0], D), jnp.float32)
    projected, unused = lax.scan(one_head, start_sum, (query_heads, key_heads, value_heads, out_heads))
    mixed = dec_states.astype(jnp.float32) + projected.reshape(dec_states.shape)
    return mixed.astype(jnp.bfloat16)
```

```python
import functools
import jax
import jax.numpy as jnp
from jax import lax
from jax.experimental import pallas as pl
from jax.experimental.pallas import tpu as pltpu
from jax.sharding import PartitionSpec as P

HD = 64
EPSILON = 1e-06
DEAD = -1e30
CHUNKS = 4
F32 = jnp.float32
BF16 = jnp.bfloat16


def norm_rows(load, store, gain, rows):
    step = 16

    def one(i, carry):
        at = pl.ds(pl.multiple_of(i * step, step), step)
        x = load(at).astype(F32)
        ms = jnp.mean(x * x, axis=-1, keepdims=True)
        store(at, (x * lax.rsqrt(ms + EPSILON) * gain).astype(BF16))
        return carry

    lax.fori_loop(0, rows // step, one, 0)


def kernel(
    cfg, qo, states, enc_gain, dec_states, dec_gain, qw, kvw, ow, out,
    gat, qw_v, kv_v, ow_v, xn, kvs, qall, a_s, e_s, psend, ssend, precv, srecv,
    att, rsend, rpart, rx, rown,
    local_sem, xs_send, xs_recv, q_send, q_recv, p_send, p_recv, s_send, s_recv,
    d_send, d_recv, r_send, r_recv,
):
    n_seq, nz, nlq, plen, dlen, width, cols = cfg
    nx = n_seq // 2
    npairs = cols // 128
    rows = nlq * dlen
    me = lax.axis_index("seq")
    z = lax.axis_index("qset")
    x = me // 2
    c = lax.rem(me, 2)
    partner = x * 2 + (1 - c)

    def seq_of(dx, core):
        return lax.rem(x + dx, nx) * 2 + core

    own_copy = pltpu.make_async_copy(states, gat.at[me], local_sem.at[0])
    own_copy.start()
    qw_copy = pltpu.make_async_copy(qw, qw_v, local_sem.at[1])
    qw_copy.start()
    kv_copy = pltpu.make_async_copy(kvw, kv_v, local_sem.at[2])
    kv_copy.start()
    ow_copy = pltpu.make_async_copy(ow, ow_v, local_sem.at[3])

    barrier = pltpu.get_barrier_semaphore()
    for dx in range(1, nx):
        pl.semaphore_signal(barrier, 1, device_id={"seq": seq_of(dx, c)})
    pl.semaphore_signal(barrier, 1, device_id={"seq": partner})
    for dz in range(1, nz):
        pl.semaphore_signal(barrier, 1, device_id={"qset": lax.rem(z + dz, nz)})
    pl.semaphore_wait(barrier, nx - 1 + 1 + nz - 1)

    own_copy.wait()
    crows = plen // CHUNKS

    def state_copy(slot, ch, to, send_sem):
        part = gat.at[slot, pl.ds(ch * crows, crows)]
        return pltpu.make_async_remote_copy(
            src_ref=part, dst_ref=part, send_sem=send_sem,
            recv_sem=xs_recv.at[slot, ch], device_id={"seq": to},
        )

    pending = []
    for ch in range(CHUNKS):
        for dx in range(1, nx):
            cp = state_copy(me, ch, seq_of(dx, c), xs_send.at[0, dx, ch])
            cp.start()
            pending.append(cp)
        cp = state_copy(me, ch, partner, xs_send.at[0, 0, ch])
        cp.start()
        pending.append(cp)

    dg = dec_gain[...].astype(F32)
    eg = enc_gain[...].astype(F32)

    def put_xn(base):
        def put(at, v):
            xn[pl.ds(pl.multiple_of(base + at.start, 16), at.size), :] = v
        return put

    norm_rows(lambda at: dec_states[at, :], put_xn(0), dg, rows)
    qw_copy.wait()
    ow_copy.start()
    tile = min(256, cols)

    def q_tile(i, carry):
        at = pl.ds(pl.multiple_of(i * tile, tile), tile)
        r = jnp.dot(xn[:rows, :], qw_v[:, at], preferred_element_type=F32).astype(BF16)
        for lq in range(nlq):
            qall[z * nlq + lq, :, at] = r[lq * dlen:(lq + 1) * dlen]
        return carry

    lax.fori_loop(0, cols // tile, q_tile, 0)
    own_q = qall.at[pl.ds(z * nlq, nlq)]
    for dz in range(1, nz):
        cp = pltpu.make_async_remote_copy(
            src_ref=own_q, dst_ref=own_q, send_sem=q_send.at[dz],
            recv_sem=q_recv.at[z], device_id={"qset": lax.rem(z + dz, nz)},
        )
        cp.start()
        pending.append(cp)

    def wait_slot(slot, ch):
        state_copy(slot, ch, partner, xs_send.at[0, 0, 0]).wait_recv()

    def project(xi):
        for k in range(2):
            norm_rows(lambda at: gat[xi * 2 + k, at, :], put_xn(k * plen), eg, plen)

        def kv_tile(i, carry):
            at = pl.ds(pl.multiple_of(i * tile, tile), tile)
            kvs[xi, :, at] = jnp.dot(
                xn[...], kv_v[:, at], preferred_element_type=F32
            ).astype(BF16)
            return carry

        lax.fori_loop(0, 2 * cols // tile, kv_tile, 0)

    for ch in range(CHUNKS):
        wait_slot(partner, ch)
    kv_copy.wait()
    project(x)
    for dx in range(1, nx):
        for ch in range(CHUNKS):
            slot = seq_of(dx, c)
            wait_slot(slot, ch)
            cp = state_copy(slot, ch, partner, xs_send.at[1, dx, ch])
            cp.start()
            pending.append(cp)
    for dx in range(1, nx):
        for ch in range(CHUNKS):
            wait_slot(seq_of(dx, 1 - c), ch)
        project(lax.rem(x + dx, nx))

    for dz in range(1, nz):
        zs = lax.rem(z + dz, nz)
        src = qall.at[pl.ds(zs * nlq, nlq)]
        pltpu.make_async_remote_copy(
            src_ref=src, dst_ref=src, send_sem=q_send.at[0],
            recv_sem=q_recv.at[zs], device_id={"qset": zs},
        ).wait_recv()

    low = lax.broadcasted_iota(jnp.int32, (dlen, 128), 1) < HD
    lane = lax.broadcasted_iota(jnp.int32, (dlen, 128), 1)

    def attend(p, carry):
        qp = qall[qo[z, p]]
        xi = p // 2
        at = pl.ds(pl.multiple_of(lax.rem(p, 2) * plen, plen), plen)
        for j in range(npairs):
            q = qp[:, j * 128:(j + 1) * 128]
            zero = jnp.zeros_like(q)
            q2 = jnp.concatenate([jnp.where(low, q, zero), jnp.where(low, zero, q)], axis=0)
            k = kvs[xi, at, pl.ds(j * 128, 128)]
            v = kvs[xi, at, pl.ds(cols + j * 128, 128)]
            s = lax.dot_general(q2, k, (((1,), (1,)), ((), ())), preferred_element_type=F32)
            m = jnp.max(s, axis=-1, keepdims=True)
            w = jnp.exp(s - m)
            l = jnp.sum(w, axis=-1, keepdims=True)
            o = jnp.dot(w.astype(BF16), v, preferred_element_type=F32) / l
            e = jnp.broadcast_to(m + jnp.log(l), o.shape)
            a_s[p, :, pl.ds(j * 128, 128)] = jnp.where(low, o[:dlen], o[dlen:])
            e_s[p, :, pl.ds(j * 128, 128)] = jnp.where(low, e[:dlen], e[dlen:])
        return carry

    lax.fori_loop(0, n_seq, attend, 0)

    for dz in list(range(1, nz)) + [0]:
        dest = lax.rem(z + dz, nz)
        packed = jnp.zeros((dlen, 128), F32)
        for lq in range(nlq):
            question = dest * nlq + lq
            first = jnp.int32(0)
            second = jnp.int32(0)
            count = jnp.int32(0)
            for p in range(n_seq):
                hit = qo[z, p] == question
                first = jnp.where(hit & (count == 0), p, first)
                second = jnp.where(hit & (count == 1), p, second)
                count = count + hit.astype(jnp.int32)
            for j in range(npairs):
                at = pl.ds(j * 128, 128)
                e1 = jnp.where(count >= 1, e_s[first, :, at], DEAD)
                e2 = jnp.where(count >= 2, e_s[second, :, at], DEAD)
                top = jnp.maximum(e1, e2)
                w1 = jnp.exp(e1 - top)
                w2 = jnp.exp(e2 - top)
                tot = w1 + w2
                a = (w1 * a_s[first, :, at] + w2 * a_s[second, :, at]) / tot
                a = jnp.where(count >= 1, a, 0.0).astype(BF16)
                le = jnp.where(count >= 1, top + jnp.log(tot), DEAD)
                packed = jnp.where((lane & (HD - 1)) == lq * npairs + j, le, packed)
                if dz == 0:
                    precv[z, pl.ds(lq * dlen, dlen), at] = a
                else:
                    psend[dz, pl.ds(lq * dlen, dlen), at] = a
        if dz == 0:
            srecv[z] = packed
        else:
            ssend[dz] = packed
            for src, dst, ss, rs in (
                (ssend, srecv, s_send, s_recv), (psend, precv, p_send, p_recv),
            ):
                cp = pltpu.make_async_remote_copy(
                    src_ref=src.at[dz], dst_ref=dst.at[z], send_sem=ss.at[dz],
                    recv_sem=rs.at[z], device_id={"qset": dest},
                )
                cp.start()
                pending.append(cp)
    for dz in range(1, nz):
        zs = lax.rem(z + dz, nz)
        for src, dst, ss, rs in (
            (ssend, srecv, s_send, s_recv), (psend, precv, p_send, p_recv),
        ):
            pltpu.make_async_remote_copy(
                src_ref=src.at[dz], dst_ref=dst.at[zs], send_sem=ss.at[0],
                recv_sem=rs.at[zs], device_id={"qset": zs},
            ).wait_recv()
    for lq in range(nlq):
        for j in range(npairs):
            at = pl.ds(j * 128, 128)
            i = lq * npairs + j
            es = []
            for zs in range(nz):
                t = srecv[zs]
                es.append(jnp.where(low, t[:, i:i + 1], t[:, HD + i:HD + i + 1]))
            top = functools.reduce(jnp.maximum, es)
            tot = jnp.zeros((dlen, 128), F32)
            acc = jnp.zeros((dlen, 128), F32)
            for zs in range(nz):
                w = jnp.exp(es[zs] - top)
                tot = tot + w
                acc = acc + w * precv[zs, pl.ds(lq * dlen, dlen), at].astype(F32)
            att[pl.ds(lq * dlen, dlen), at] = (acc / tot).astype(BF16)

    ow_copy.wait()
    piece = width // n_seq
    ptile = min(256, piece)

    def project_out(dest, put):
        def one(i, carry):
            src = pl.ds(pl.multiple_of(dest * piece + i * ptile, 128), ptile)
            at = pl.ds(pl.multiple_of(i * ptile, ptile), ptile)
            put(at, src, jnp.dot(att[...], ow_v[:, src], preferred_element_type=F32))
            return carry

        lax.fori_loop(0, piece // ptile, one, 0)

    order = list(range(1, nx)) + [0]
    for dx in order:
        def put_send(at, src, r):
            rsend[dx, :, at] = r.astype(BF16)

        project_out(seq_of(dx, 1 - c), put_send)
        cp = pltpu.make_async_remote_copy(
            src_ref=rsend.at[dx], dst_ref=rpart.at[dx], send_sem=d_send.at[dx],
            recv_sem=d_recv.at[dx], device_id={"seq": partner},
        )
        cp.start()
        pending.append(cp)

    def wait_part(dx):
        pltpu.make_async_remote_copy(
            src_ref=rsend.at[dx], dst_ref=rpart.at[dx], send_sem=d_send.at[dx],
            recv_sem=d_recv.at[dx], device_id={"seq": partner},
        ).wait_recv()

    for dx in order:
        def put_sum(at, src, r):
            rown[:, at] = r

        project_out(seq_of(dx, c), put_sum)
        wait_part(dx)
        if dx:
            rsend[nx + dx] = (rown[...] + rpart[dx].astype(F32)).astype(BF16)
            cp = pltpu.make_async_remote_copy(
                src_ref=rsend.at[nx + dx], dst_ref=rx.at[x], send_sem=r_send.at[dx],
                recv_sem=r_recv.at[x], device_id={"seq": seq_of(dx, c)},
            )
            cp.start()
            pending.append(cp)
        else:
            mine = pl.ds(pl.multiple_of(me * piece, 128), piece)
            rown[...] = rown[...] + rpart[0].astype(F32) + dec_states[:, mine].astype(F32)
    total = rown[...]
    for dx in range(1, nx):
        xs = lax.rem(x + dx, nx)
        pltpu.make_async_remote_copy(
            src_ref=rsend.at[0], dst_ref=rx.at[xs], send_sem=r_send.at[0],
            recv_sem=r_recv.at[xs], device_id={"seq": xs * 2 + c},
        ).wait_recv()
        total = total + rx[xs].astype(F32)
    out[...] = total.astype(BF16)
    for cp in pending:
        cp.wait_send()


def body(
    states, enc_gain, dec_states, dec_gain, query_weight, key_value_weight, out_weight, question_of
):
    nz = lax.axis_size("qset")
    n_seq = lax.axis_size("seq")
    nx = n_seq // 2
    plen, width = states.shape[2], states.shape[3]
    nlq, dlen = dec_states.shape[0], dec_states.shape[1]
    cols = query_weight.shape[1]
    rows = nlq * dlen
    piece = width // n_seq
    cfg = (n_seq, nz, nlq, plen, dlen, width, cols)
    any_spec = pl.BlockSpec(memory_space=pl.ANY)
    vmem = pl.BlockSpec(memory_space=pltpu.VMEM)
    dma = pltpu.SemaphoreType.DMA
    result = pl.pallas_call(
        functools.partial(kernel, cfg),
        out_shape=jax.ShapeDtypeStruct((rows, piece), BF16),
        in_specs=[pl.BlockSpec(memory_space=pltpu.SMEM), any_spec, vmem, vmem, vmem,
                  any_spec, any_spec, any_spec],
        out_specs=vmem,
        scratch_shapes=[
            pltpu.VMEM((n_seq, plen, width), BF16),
            pltpu.VMEM((width, cols), BF16),
            pltpu.VMEM((width, 2 * cols), BF16),
            pltpu.VMEM((cols, width), BF16),
            pltpu.VMEM((2 * plen, width), BF16),
            pltpu.VMEM((nx, 2 * plen, 2 * cols), BF16),
            pltpu.VMEM((nlq * nz, dlen, cols), BF16),
            pltpu.VMEM((n_seq, dlen, cols), F32),
            pltpu.VMEM((n_seq, dlen, cols), F32),
            pltpu.VMEM((nz, rows, cols), BF16),
            pltpu.VMEM((nz, dlen, 128), F32),
            pltpu.VMEM((nz, rows, cols), BF16),
            pltpu.VMEM((nz, dlen, 128), F32),
            pltpu.VMEM((rows, cols), BF16),
            pltpu.VMEM((2 * nx, rows, piece), BF16),
            pltpu.VMEM((nx, rows, piece), BF16),
            pltpu.VMEM((nx, rows, piece), BF16),
            pltpu.VMEM((rows, piece), F32),
            dma((4,)),
            dma((2, nx, CHUNKS)), dma((n_seq, CHUNKS)),
            dma((nz,)), dma((nz,)), dma((nz,)), dma((nz,)), dma((nz,)), dma((nz,)),
            dma((nx,)), dma((nx,)), dma((nx,)), dma((nx,)),
        ],
        compiler_params=pltpu.CompilerParams(
            collective_id=0, has_side_effects=True, vmem_limit_bytes=63 * 1024 * 1024
        ),
        name="reader",
    )(
        question_of[:, :, 0], states.reshape(plen, width), enc_gain.reshape(1, width),
        dec_states.reshape(rows, width), dec_gain.reshape(1, width),
        query_weight, key_value_weight.reshape(width, 2 * cols), out_weight,
    )
    return result.reshape(nlq, dlen, piece)


def solution(mesh):
    return jax.shard_map(
        body,
        mesh=mesh,
        in_specs=(
            P(("groups", "qset"), "seq", None, None),
            P(),
            P(("groups", "qset"), None, None),
            P(),
            P(None, "seq"),
            P(None, None, "seq"),
            P("seq", None),
            P("groups", None, None),
        ),
        out_specs=P(("groups", "qset"), None, "seq"),
        check_vma=False,
    )
```

```python
import functools
import jax
import jax.numpy as jnp
from jax import lax
from jax.experimental import pallas as pl
from jax.experimental.pallas import tpu as pltpu
from jax.sharding import PartitionSpec as P

HD = 64
EPSILON = 1e-06
DEAD = -1e30
CHUNKS = 4
F32 = jnp.float32
BF16 = jnp.bfloat16


def norm_rows(load, store, gain, rows):
    step = 16

    def one(i, carry):
        at = pl.ds(pl.multiple_of(i * step, step), step)
        x = load(at).astype(F32)
        ms = jnp.mean(x * x, axis=-1, keepdims=True)
        store(at, (x * lax.rsqrt(ms + EPSILON) * gain).astype(BF16))
        return carry

    lax.fori_loop(0, rows // step, one, 0)


def kernel(
    cfg, qo, states, enc_gain, dec_states, dec_gain, qw, kvw, ow, out,
    gat, qw_v, raw, pulled, kv_v, ow_v, xn, kvs, qall, a_s, e_s, psend, ssend, precv, srecv,
    att, oacc, rsend, rpart, rx, rown,
    local_sem, raw_sem, xs_send, xs_recv, q_send, q_recv, p_send, p_recv, s_send, s_recv,
    d_send, d_recv, r_send, r_recv,
):
    n_seq, nz, nlq, plen, dlen, width, cols = cfg
    nx = n_seq // 2
    npairs = cols // 128
    rows = nlq * dlen
    nch = 4 if npairs % 4 == 0 else npairs
    pc = npairs // nch
    cw = pc * 128
    me = lax.axis_index("seq")
    z = lax.axis_index("qset")
    x = me // 2
    c = lax.rem(me, 2)
    partner = x * 2 + (1 - c)

    def seq_of(dx, core):
        return lax.rem(x + dx, nx) * 2 + core

    own_copy = pltpu.make_async_copy(states, gat.at[me], local_sem.at[0])
    own_copy.start()
    qw_copy = pltpu.make_async_copy(qw, qw_v, local_sem.at[1])
    qw_copy.start()
    nblocks = cols // 128
    slots = raw.shape[0]

    def raw_copy(b):
        return pltpu.make_async_copy(
            kvw.at[:, :, pl.ds(b * 128, 128)], raw.at[b % slots], raw_sem.at[b % slots]
        )

    for b in range(min(slots, nblocks)):
        raw_copy(b).start()
    ow_copy = pltpu.make_async_copy(ow, ow_v, local_sem.at[3])

    barrier = pltpu.get_barrier_semaphore()
    for dx in range(1, nx):
        pl.semaphore_signal(barrier, 1, device_id={"seq": seq_of(dx, c)})
    pl.semaphore_signal(barrier, 1, device_id={"seq": partner})
    for dz in range(1, nz):
        pl.semaphore_signal(barrier, 1, device_id={"qset": lax.rem(z + dz, nz)})
    pl.semaphore_wait(barrier, nx - 1 + 1 + nz - 1)

    own_copy.wait()
    crows = plen // CHUNKS

    def state_copy(slot, ch, to, send_sem):
        part = gat.at[slot, pl.ds(ch * crows, crows)]
        return pltpu.make_async_remote_copy(
            src_ref=part, dst_ref=part, send_sem=send_sem,
            recv_sem=xs_recv.at[slot, ch], device_id={"seq": to},
        )

    pending = []
    for ch in range(CHUNKS):
        for dx in range(1, nx):
            cp = state_copy(me, ch, seq_of(dx, c), xs_send.at[0, dx, ch])
            cp.start()
            pending.append(cp)
        cp = state_copy(me, ch, partner, xs_send.at[0, 0, ch])
        cp.start()
        pending.append(cp)

    dg = dec_gain[...].astype(F32).reshape(1, width)
    eg = enc_gain[...].astype(F32).reshape(1, width)

    def put_xn(base):
        def put(at, v):
            xn[pl.ds(pl.multiple_of(base + at.start, 16), at.size), :] = v
        return put

    norm_rows(lambda at: dec_states[at, :], put_xn(0), dg, rows)
    qw_copy.wait()
    ow_copy.start()
    tile = min(256, cols)

    def q_tile(i, carry):
        at = pl.ds(pl.multiple_of(i * tile, tile), tile)
        r = jnp.dot(xn[:rows, :], qw_v[:, at], preferred_element_type=F32).astype(BF16)
        for lq in range(nlq):
            qall[z * nlq + lq, :, at] = r[lq * dlen:(lq + 1) * dlen]
        return carry

    lax.fori_loop(0, cols // tile, q_tile, 0)
    own_q = qall.at[pl.ds(z * nlq, nlq)]
    for dz in range(1, nz):
        cp = pltpu.make_async_remote_copy(
            src_ref=own_q, dst_ref=own_q, send_sem=q_send.at[dz],
            recv_sem=q_recv.at[z], device_id={"qset": lax.rem(z + dz, nz)},
        )
        cp.start()
        pending.append(cp)

    def wait_slot(slot, ch):
        state_copy(slot, ch, partner, xs_send.at[0, 0, 0]).wait_recv()

    def project(xi, start, count):
        for k in range(2):
            norm_rows(
                lambda at: gat[xi * 2 + k, pl.ds(pl.multiple_of(start + at.start, 16), at.size), :],
                put_xn(k * count), eg, count,
            )

        def kv_tile(i, carry):
            at = pl.ds(pl.multiple_of(i * tile, tile), tile)
            r = jnp.dot(
                xn[:2 * count, :], kv_v[:, at], preferred_element_type=F32
            ).astype(BF16)
            for k in range(2):
                kvs[xi, pl.ds(k * plen + start, count), at] = r[k * count:(k + 1) * count]
            return carry

        lax.fori_loop(0, 2 * cols // tile, kv_tile, 0)

    def forward(ch):
        for dx in range(1, nx):
            slot = seq_of(dx, c)
            wait_slot(slot, ch)
            cp = state_copy(slot, ch, partner, xs_send.at[1, dx, ch])
            cp.start()
            pending.append(cp)

    half = pulled.shape[0] // 2
    for b in range(nblocks):
        raw_copy(b).wait()
        flat = raw.at[b % slots].reshape(2 * width, 128)

        def pull(i, carry):
            pulled[...] = flat[pl.ds(pl.multiple_of(i * 2 * half, 2 * half), 2 * half), :].astype(F32)
            at = pl.ds(pl.multiple_of(i * half, half), half)
            kv_v[at, pl.ds(b * 128, 128)] = pulled[pl.ds(0, half, stride=2), :].astype(BF16)
            kv_v[at, pl.ds(cols + b * 128, 128)] = pulled[pl.ds(1, half, stride=2), :].astype(BF16)
            return carry

        lax.fori_loop(0, width // half, pull, 0)
        if b + slots < nblocks:
            raw_copy(b + slots).start()
        if b == nblocks // 2:
            forward(0)

    for ch in range(CHUNKS):
        wait_slot(partner, ch)
    forward(1)
    project(x, 0, plen)
    forward(2)
    part = plen // 2
    for dx in range(1, nx):
        for ch in range(CHUNKS // 2):
            wait_slot(seq_of(dx, 1 - c), ch)
        project(lax.rem(x + dx, nx), 0, part)
    forward(3)
    for dx in range(1, nx):
        for ch in range(CHUNKS // 2, CHUNKS):
            wait_slot(seq_of(dx, 1 - c), ch)
        project(lax.rem(x + dx, nx), part, part)

    for dz in range(1, nz):
        zs = lax.rem(z + dz, nz)
        src = qall.at[pl.ds(zs * nlq, nlq)]
        pltpu.make_async_remote_copy(
            src_ref=src, dst_ref=src, send_sem=q_send.at[0],
            recv_sem=q_recv.at[zs], device_id={"qset": zs},
        ).wait_recv()

    low = lax.broadcasted_iota(jnp.int32, (dlen, 128), 1) < HD
    lane = lax.broadcasted_iota(jnp.int32, (dlen, 128), 1)

    groups = dlen // 8

    def attend(g, p):
        qp = qall[qo[z, p], :, pl.ds(g * cw, cw)]
        xi = p // 2
        at = pl.ds(pl.multiple_of(lax.rem(p, 2) * plen, plen), plen)
        for i in range(pc):
            j = g * pc + i
            q = qp[:, i * 128:(i + 1) * 128]
            zero = jnp.zeros_like(q)
            q2 = jnp.concatenate([jnp.where(low, q, zero), jnp.where(low, zero, q)], axis=0)
            k = kvs[xi, at, pl.ds(j * 128, 128)]
            v = kvs[xi, at, pl.ds(cols + j * 128, 128)]
            s = lax.dot_general(q2, k, (((1,), (1,)), ((), ())), preferred_element_type=F32)
            m = jnp.max(s, axis=-1, keepdims=True)
            w = jnp.exp(s - m)
            l = jnp.sum(w, axis=-1, keepdims=True)
            o = jnp.dot(w.astype(BF16), v, preferred_element_type=F32) / l
            e = jnp.broadcast_to(m + jnp.log(l), o.shape)
            a_s[p, :, pl.ds(i * 128, 128)] = jnp.where(low, o[:dlen], o[dlen:])
            e_s[p, :, pl.ds(i * 128, 128)] = jnp.where(low, e[:dlen], e[dlen:])

    def exchange(g, dz, sender):
        zs = lax.rem(z + dz, nz)
        to = z if sender else zs
        return [
            pltpu.make_async_remote_copy(
                src_ref=src.at[g, dz], dst_ref=dst.at[g, to], send_sem=ss.at[g, dz],
                recv_sem=rs.at[g, to], device_id={"qset": zs},
            )
            for src, dst, ss, rs in (
                (ssend, srecv, s_send, s_recv), (psend, precv, p_send, p_recv),
            )
        ]

    for g in range(nch):
        lax.fori_loop(0, n_seq, lambda p, carry: (attend(g, p), carry)[1], 0, unroll=4)
        for dz in list(range(1, nz)) + [0]:
            dest = lax.rem(z + dz, nz)
            packed = jnp.zeros((dlen, 128), F32)
            for lq in range(nlq):
                question = dest * nlq + lq
                first = jnp.int32(0)
                second = jnp.int32(0)
                count = jnp.int32(0)
                for p in range(n_seq):
                    hit = qo[z, p] == question
                    first = jnp.where(hit & (count == 0), p, first)
                    second = jnp.where(hit & (count == 1), p, second)
                    count = count + hit.astype(jnp.int32)
                for i in range(pc):
                    at = pl.ds(i * 128, 128)
                    e1 = jnp.where(count >= 1, e_s[first, :, at], DEAD)
                    e2 = jnp.where(count >= 2, e_s[second, :, at], DEAD)
                    top = jnp.maximum(e1, e2)
                    w1 = jnp.exp(e1 - top)
                    w2 = jnp.exp(e2 - top)
                    tot = w1 + w2
                    a = (w1 * a_s[first, :, at] + w2 * a_s[second, :, at]) / tot
                    a = jnp.where(count >= 1, a, 0.0).astype(BF16)
                    le = jnp.where(count >= 1, top + jnp.log(tot), DEAD)
                    packed = jnp.where((lane & (HD - 1)) == lq * pc + i, le, packed)
                    if dz == 0:
                        precv[g, z, pl.ds(lq * dlen, dlen), at] = a
                    else:
                        psend[g, dz, pl.ds(lq * dlen, dlen), at] = a
            tight = jnp.zeros((8, 128), F32)
            for t in range(groups):
                piece8 = packed[t * 8:(t + 1) * 8]
                tight = tight + (pltpu.roll(piece8, t * 8, 1) if t else piece8)
            if dz == 0:
                srecv[g, z] = tight
            else:
                ssend[g, dz] = tight
                for cp in exchange(g, dz, True):
                    cp.start()
                    pending.append(cp)
    ow_copy.wait()
    otile = min(256, width // n_seq)
    for g in range(nch):
        for dz in range(1, nz):
            for cp in exchange(g, dz, False):
                cp.wait_recv()
        spread = []
        for zs in range(nz):
            t8 = srecv[g, zs]
            spread.append(jnp.concatenate(
                [pltpu.roll(t8, 128 - t * 8, 1) if t else t8 for t in range(groups)], axis=0))
        for lq in range(nlq):
            for i in range(pc):
                at = pl.ds(i * 128, 128)
                n = lq * pc + i
                es = [jnp.where(low, t[:, n:n + 1], t[:, HD + n:HD + n + 1]) for t in spread]
                top = functools.reduce(jnp.maximum, es)
                tot = jnp.zeros((dlen, 128), F32)
                acc = jnp.zeros((dlen, 128), F32)
                for zs in range(nz):
                    w = jnp.exp(es[zs] - top)
                    tot = tot + w
                    acc = acc + w * precv[g, zs, pl.ds(lq * dlen, dlen), at].astype(F32)
                att[g, pl.ds(lq * dlen, dlen), at] = (acc / tot).astype(BF16)
        if g < nch - 1:
            def early(i, carry):
                at = pl.ds(pl.multiple_of(i * otile, otile), otile)
                r = jnp.dot(
                    att[g], ow_v[pl.ds(g * cw, cw), at], preferred_element_type=F32
                )
                oacc[:, at] = r if g == 0 else oacc[:, at] + r
                return carry

            lax.fori_loop(0, width // otile, early, 0)

    piece = width // n_seq
    ptile = min(256, piece)

    def project_out(dest, put):
        def one(i, carry):
            src = pl.ds(pl.multiple_of(dest * piece + i * ptile, 128), ptile)
            at = pl.ds(pl.multiple_of(i * ptile, ptile), ptile)
            r = jnp.dot(
                att[nch - 1], ow_v[pl.ds((nch - 1) * cw, cw), src], preferred_element_type=F32
            )
            put(at, src, oacc[:, src] + r if nch > 1 else r)
            return carry

        lax.fori_loop(0, piece // ptile, one, 0)

    order = list(range(1, nx)) + [0]
    for dx in order:
        def put_send(at, src, r):
            rsend[dx, :, at] = r.astype(BF16)

        project_out(seq_of(dx, 1 - c), put_send)
        cp = pltpu.make_async_remote_copy(
            src_ref=rsend.at[dx], dst_ref=rpart.at[dx], send_sem=d_send.at[dx],
            recv_sem=d_recv.at[dx], device_id={"seq": partner},
        )
        cp.start()
        pending.append(cp)

    def wait_part(dx):
        pltpu.make_async_remote_copy(
            src_ref=rsend.at[dx], dst_ref=rpart.at[dx], send_sem=d_send.at[dx],
            recv_sem=d_recv.at[dx], device_id={"seq": partner},
        ).wait_recv()

    for dx in order:
        def put_sum(at, src, r):
            rown[:, at] = r

        project_out(seq_of(dx, c), put_sum)
        wait_part(dx)
        if dx:
            rsend[nx + dx] = (rown[...] + rpart[dx].astype(F32)).astype(BF16)
            cp = pltpu.make_async_remote_copy(
                src_ref=rsend.at[nx + dx], dst_ref=rx.at[x], send_sem=r_send.at[dx],
                recv_sem=r_recv.at[x], device_id={"seq": seq_of(dx, c)},
            )
            cp.start()
            pending.append(cp)
        else:
            mine = pl.ds(pl.multiple_of(me * piece, 128), piece)
            rown[...] = rown[...] + rpart[0].astype(F32) + dec_states[:, mine].astype(F32)
    total = rown[...]
    for dx in range(1, nx):
        xs = lax.rem(x + dx, nx)
        pltpu.make_async_remote_copy(
            src_ref=rsend.at[0], dst_ref=rx.at[xs], send_sem=r_send.at[0],
            recv_sem=r_recv.at[xs], device_id={"seq": xs * 2 + c},
        ).wait_recv()
        total = total + rx[xs].astype(F32)
    out[...] = total.astype(BF16)
    for cp in pending:
        cp.wait_send()


def body(
    states, enc_gain, dec_states, dec_gain, query_weight, key_value_weight, out_weight, question_of
):
    nz = lax.axis_size("qset")
    n_seq = lax.axis_size("seq")
    nx = n_seq // 2
    plen, width = states.shape[2], states.shape[3]
    nlq, dlen = dec_states.shape[0], dec_states.shape[1]
    cols = query_weight.shape[1]
    rows = nlq * dlen
    piece = width // n_seq
    npairs = cols // 128
    nch = 4 if npairs % 4 == 0 else npairs
    cw = cols // nch
    cfg = (n_seq, nz, nlq, plen, dlen, width, cols)
    any_spec = pl.BlockSpec(memory_space=pl.ANY)
    vmem = pl.BlockSpec(memory_space=pltpu.VMEM)
    dma = pltpu.SemaphoreType.DMA
    result = pl.pallas_call(
        functools.partial(kernel, cfg),
        out_shape=jax.ShapeDtypeStruct((rows, piece), BF16),
        in_specs=[pl.BlockSpec(memory_space=pltpu.SMEM), any_spec, vmem, vmem, vmem,
                  any_spec, any_spec, any_spec],
        out_specs=vmem,
        scratch_shapes=[
            pltpu.VMEM((n_seq, plen, width), BF16),
            pltpu.VMEM((width, cols), BF16),
            pltpu.VMEM((2, width, 2, 128), BF16),
            pltpu.VMEM((1024, 128), F32),
            pltpu.VMEM((width, 2 * cols), BF16),
            pltpu.VMEM((cols, width), BF16),
            pltpu.VMEM((2 * plen, width), BF16),
            pltpu.VMEM((nx, 2 * plen, 2 * cols), BF16),
            pltpu.VMEM((nlq * nz, dlen, cols), BF16),
            pltpu.VMEM((n_seq, dlen, cw), F32),
            pltpu.VMEM((n_seq, dlen, cw), F32),
            pltpu.VMEM((nch, nz, rows, cw), BF16),
            pltpu.VMEM((nch, nz, 8, 128), F32),
            pltpu.VMEM((nch, nz, rows, cw), BF16),
            pltpu.VMEM((nch, nz, 8, 128), F32),
            pltpu.VMEM((nch, rows, cw), BF16),
            pltpu.VMEM((rows, width), F32),
            pltpu.VMEM((2 * nx, rows, piece), BF16),
            pltpu.VMEM((nx, rows, piece), BF16),
            pltpu.VMEM((nx, rows, piece), BF16),
            pltpu.VMEM((rows, piece), F32),
            dma((4,)), dma((2,)),
            dma((2, nx, CHUNKS)), dma((n_seq, CHUNKS)),
            dma((nz,)), dma((nz,)),
            dma((nch, nz)), dma((nch, nz)), dma((nch, nz)), dma((nch, nz)),
            dma((nx,)), dma((nx,)), dma((nx,)), dma((nx,)),
        ],
        compiler_params=pltpu.CompilerParams(
            collective_id=0, has_side_effects=True, vmem_limit_bytes=63 * 1024 * 1024
        ),
        name="reader",
    )(
        question_of[:, :, 0], states.reshape(plen, width), enc_gain,
        dec_states.reshape(rows, width), dec_gain,
        query_weight, key_value_weight, out_weight,
    )
    return result.reshape(nlq, dlen, piece)


def solution(mesh):
    return jax.shard_map(
        body,
        mesh=mesh,
        in_specs=(
            P(("groups", "qset"), "seq", None, None),
            P(),
            P(("groups", "qset"), None, None),
            P(),
            P(None, "seq"),
            P(None, None, "seq"),
            P("seq", None),
            P("groups", None, None),
        ),
        out_specs=P(("groups", "qset"), None, "seq"),
        check_vma=False,
    )
```
